32 devices in a mesh: tm: 16 (over z, y, core), asset: 2 (over x).
Axes of the slice: x: 2, y: 2, z: 4, core: 2. Of those that a mesh axis runs over, the one named last changes fastest.
Arguments:
- tick_bars: float32 [2, 16, 61440], P('asset', 'tm'), may hold values from -20 to 20
- prior_bars: float32 [2, 16, 6400], P('asset', 'tm'), may hold values from -20 to 20, as said below
Outputs:
- connectedness: float32 [48, 8192], P('tm', 'asset')
The draws below stay inside these ranges and needn't reach their ends.
Inputs may be any that keep to these rules, and one draw needn't show every extreme that they name: `prior_bars`: bar returns of the same assets.
All inputs are finite; a program needn't handle non-finite values.
Results may differ from the reference program's by a relative error of at most 0.0014.
Values may be sent and summed in bfloat16 or wider, within the bound.
A program may use at most 64 MiB of HBM per device.

```python
import math
import jax
import jax.numpy as jnp
from jax import lax

ASSETS = 8192
SPAN = 30
STRIDE = 5
LEAD = 25
BARS = 240
WINDOWS = 48
N_TM = 16


cluster_count = 16


def return_draw(key, count, salt):
    tile_cols = ASSETS // 2
    log_scale = jax.random.uniform(jax.random.fold_in(key, 11), (2, 1, tile_cols), jnp.float32, math.log(0.1), math.log(3.0))
    scales = jnp.exp(log_scale)
    first_pick = jax.random.randint(jax.random.fold_in(key, 13), (2, tile_cols), 0, cluster_count)
    second_pick = jax.random.randint(jax.random.fold_in(key, 14), (2, tile_cols), 0, cluster_count)
    cluster = jnp.minimum(first_pick, second_pick)
    signs = 2.0 * jax.random.randint(jax.random.fold_in(key, 15), (2, 1, tile_cols), 0, 2).astype(jnp.float32) - 1.0
    loading = signs * jax.random.uniform(jax.random.fold_in(key, 16), (2, 1, tile_cols), jnp.float32, 0.3, 1.3)
    noise_key = jax.random.fold_in(key, salt)
    sector_moves = jnp.clip(jax.random.normal(jax.random.fold_in(noise_key, 3), (count, cluster_count), jnp.float32), -3.0, 3.0)
    sector_vol = jnp.exp(jax.random.uniform(jax.random.fold_in(noise_key, 4), (count, cluster_count), jnp.float32, math.log(0.4), math.log(2.0)))
    sector_factor = sector_moves * sector_vol
    asset_factor = jnp.transpose(sector_factor[:, cluster], (1, 0, 2))
    idiosyncratic = jnp.clip(jax.random.normal(noise_key, (2, count, tile_cols), jnp.float32), -4.0, 4.0)
    drawn = scales * (loading * asset_factor + idiosyncratic)
    drawn = jnp.clip(drawn, -19.5, 19.5)
    group_cols = ASSETS // (2 * N_TM)
    grid = drawn.reshape(2, count, N_TM, group_cols)
    return jnp.transpose(grid, (0, 2, 1, 3)).reshape(2, N_TM, count * group_cols).astype(jnp.float32)


def draw_tick_bars(key, part):
    return return_draw(key, BARS, 21)


def draw_prior_bars(key, part):
    return return_draw(key, LEAD, 22)


def setup_inputs(seed: int = 0) -> dict:
    streams_of = jax.random.split(jax.random.key(seed), 3)
    return {
        "tick_bars": draw_tick_bars(jax.random.fold_in(streams_of[2], 71), 0),
        "prior_bars": draw_prior_bars(jax.random.fold_in(streams_of[2], 71), 0),
    }


FLOOR_SQUARES = 1.0

def standardize(values):
    centred = values - lax.optimization_barrier(jnp.mean(values, axis=0, keepdims=True))
    squares = lax.optimization_barrier(jnp.sum(centred * centred, axis=0, keepdims=True))
    return (centred * lax.rsqrt(jnp.maximum(squares, FLOOR_SQUARES))).astype(jnp.bfloat16)

def unfold(packed, count):
    group_cols = ASSETS // (2 * N_TM)
    grid = packed.reshape(2, N_TM, count, group_cols)
    return jnp.transpose(grid, (2, 0, 1, 3)).reshape(count, ASSETS)

def reference(tick_bars, prior_bars):
    series_now = unfold(tick_bars, BARS)
    series_prior = unfold(prior_bars, LEAD)
    series = jnp.concatenate([series_prior, series_now], axis=0)
    block_rows = min(2048, ASSETS)

    def one_window(window_index):
        values = lax.dynamic_slice_in_dim(series, window_index * STRIDE, SPAN, 0)
        scaled = standardize(values).astype(jnp.float32)
        pieces = []
        for offset in range(0, ASSETS, block_rows):
            correlation = jnp.dot(scaled[:, offset:offset + block_rows].T, scaled, preferred_element_type=jnp.float32)
            magnitude = jnp.abs(correlation.astype(jnp.bfloat16)).astype(jnp.float32)
            pieces.append(lax.optimization_barrier(jnp.sum(magnitude, axis=1)))
        return jnp.concatenate(pieces) * (math.sqrt(SPAN) / ASSETS)
    return lax.map(one_window, jnp.arange(WINDOWS, dtype=jnp.int32))
```

```python
import math

import jax
import jax.numpy as jnp
from jax import lax
from jax.sharding import PartitionSpec as P

ASSETS = 8192
SPAN = 30
STRIDE = 5
WIN_DEV = 3
LEAD = 25


FLOOR_SQUARES = 1.0


def swapped(block, axis, distance):
    count = lax.axis_size(axis)
    route = []
    for low in range(count):
        high = low | 1 << distance
        if high != low and high < count:
            route += [(low, high), (high, low)]
    return lax.ppermute(block, axis, route)


def window_stack(extended):
    columns = extended.shape[1]
    count = (extended.shape[0] - SPAN) // STRIDE + 1
    groups = extended.reshape(-1, STRIDE, columns)
    stacked = jnp.stack(
        [groups[offset : offset + count] for offset in range(SPAN // STRIDE)], axis=1
    )
    values = stacked.reshape(count, SPAN, columns)
    centred = values - jnp.mean(values, axis=1, keepdims=True)
    squares = jnp.sum(centred * centred, axis=1, keepdims=True)
    return (centred * lax.rsqrt(jnp.maximum(squares, FLOOR_SQUARES))).astype(jnp.bfloat16)


def block_magnitude(left_part, right_part, offset, block_rows):
    correlation = lax.dot_general(
        left_part[:, offset : offset + block_rows],
        right_part,
        (((0,), (0,)), ((), ())),
        preferred_element_type=jnp.float32,
    )
    return jnp.abs(correlation.astype(jnp.bfloat16)).astype(jnp.float32)


def row_totals(own_windows, other_windows):
    columns = own_windows.shape[2]
    block_rows = min(1024, columns)

    def row_one_window(operands):
        left_part, right_part = operands
        pieces = [
            jnp.sum(block_magnitude(left_part, right_part, offset, block_rows), axis=1)
            for offset in range(0, columns, block_rows)
        ]
        return jnp.concatenate(pieces)

    return lax.map(row_one_window, (own_windows, other_windows))


def both_totals(own_windows, other_windows):
    columns = own_windows.shape[2]
    block_rows = min(1024, columns)

    def both_one_window(operands):
        left_part, right_part = operands
        pieces = []
        column_total = jnp.zeros((right_part.shape[1],), jnp.float32)
        for offset in range(0, columns, block_rows):
            magnitude = block_magnitude(left_part, right_part, offset, block_rows)
            pieces.append(jnp.sum(magnitude, axis=1))
            column_total = column_total + jnp.sum(magnitude, axis=0)
        return (jnp.concatenate(pieces), column_total)

    return lax.map(both_one_window, (own_windows, other_windows))


def local_windows(tick_bars, prior_bars):
    groups = lax.axis_size("tm")
    group_cols = ASSETS // (2 * groups)
    series = jnp.concatenate(
        [prior_bars.reshape(-1, group_cols), tick_bars.reshape(-1, group_cols)], axis=0
    )
    return window_stack(series)


def shards(tick_bars, prior_bars):
    groups = lax.axis_size("tm")
    outgoing = local_windows(tick_bars, prior_bars)
    arrived = lax.all_to_all(outgoing, "tm", split_axis=0, concat_axis=0, tiled=True)
    arrived = arrived.reshape(groups, WIN_DEV, SPAN, -1)
    scaled = jnp.transpose(arrived, (1, 2, 0, 3)).reshape(WIN_DEV, SPAN, -1)
    columns = scaled.shape[2]
    empty = jnp.zeros((WIN_DEV, columns), jnp.float32)
    partner = swapped(scaled, "asset", 0)
    tile_index = lax.axis_index("asset")
    quarter = columns // 2
    diagonal_part = row_totals(scaled, scaled)
    column_part = empty
    cross_rows = []
    for half_index in range(2):
        mine = scaled[:, :, half_index * quarter : (half_index + 1) * quarter]
        target = (half_index + tile_index) % 2
        theirs = lax.dynamic_slice_in_dim(partner, target * quarter, quarter, 2)
        row_add, column_add = both_totals(mine, theirs)
        cross_rows.append(row_add)
        column_part = lax.dynamic_update_slice_in_dim(column_part, column_add, target * quarter, 1)
    returned = swapped(column_part.astype(jnp.bfloat16), "asset", 0).astype(column_part.dtype)
    totals = diagonal_part + jnp.concatenate(cross_rows, axis=1) + returned
    return totals * (math.sqrt(SPAN) / ASSETS)


def solution(mesh):
    in_specs = (P("asset", "tm", None), P("asset", "tm", None))
    out_specs = P("tm", "asset")
    return jax.shard_map(shards, mesh=mesh, in_specs=in_specs, out_specs=out_specs, check_vma=False)
```

```python
import math

import jax
import jax.numpy as jnp
from jax import lax
from jax.experimental import pallas as pl
from jax.experimental.pallas import tpu as pltpu
from jax.sharding import PartitionSpec as P

ASSETS = 8192
SPAN = 30
STRIDE = 5
WIN_DEV = 3
LEAD = 25
DEPTH = 32
TILE = 256
LANES = 128
SUBLANES = 8


FLOOR_SQUARES = 1.0


def swapped(block, axis, distance):
    count = lax.axis_size(axis)
    route = []
    for low in range(count):
        high = low | 1 << distance
        if high != low and high < count:
            route += [(low, high), (high, low)]
    return lax.ppermute(block, axis, route)


def window_stack(extended):
    columns = extended.shape[1]
    count = (extended.shape[0] - SPAN) // STRIDE + 1
    groups = extended.reshape(-1, STRIDE, columns)
    stacked = jnp.stack(
        [groups[offset : offset + count] for offset in range(SPAN // STRIDE)], axis=1
    )
    values = stacked.reshape(count, SPAN, columns)
    centred = values - jnp.mean(values, axis=1, keepdims=True)
    squares = jnp.sum(centred * centred, axis=1, keepdims=True)
    scaled = (centred * lax.rsqrt(jnp.maximum(squares, FLOOR_SQUARES))).astype(jnp.bfloat16)
    return jnp.pad(scaled, ((0, 0), (0, DEPTH - SPAN), (0, 0)))


def strip_totals(rows_t, source, start, width, column_sums, own_first):
    rows = rows_t.shape[0]
    row_partial = jnp.zeros((rows, LANES), jnp.float32)
    for offset in range(0, width, TILE):
        at = pl.ds(pl.multiple_of(start + offset, TILE), TILE)
        magnitude = jnp.abs(jnp.dot(rows_t, source[:, at], preferred_element_type=jnp.float32))
        row_partial = row_partial + (magnitude[:, :LANES] + magnitude[:, LANES:])
        if offset or not own_first:
            folded = jnp.sum(magnitude.reshape(rows // SUBLANES, SUBLANES, TILE), axis=0)
            column_sums[:, at] = column_sums[:, at] + folded
    return row_partial


def row_vector(row_partial):
    return jnp.sum(row_partial.T, axis=0, keepdims=True)


def diagonal_kernel(own, out, wrapped, column_sums):
    columns = own.shape[2]
    half = columns // 2
    wrapped[:, :columns] = own[0]
    wrapped[:, columns:] = own[0, :, : wrapped.shape[1] - columns]
    column_sums[...] = jnp.zeros_like(column_sums)

    def step(index, carry):
        for upper in range(2):
            first = pl.multiple_of(index * TILE + upper * half, TILE)
            rows_t = wrapped[:, pl.ds(first, TILE)].T
            width = half if upper else half + TILE
            partial = strip_totals(rows_t, wrapped, first, width, column_sums, True)
            out[0, :, pl.ds(first, TILE)] = row_vector(partial)
        return carry

    lax.fori_loop(0, half // TILE, step, 0)
    folded = jnp.sum(column_sums[...], axis=0, keepdims=True)
    out[0] = out[0] + folded[:, :columns]
    spill = columns - half
    out[0, :, :spill] = out[0, :, :spill] + folded[:, columns : columns + spill]


def cross_kernel(tile, own, other, row_out, column_out, column_sums):
    columns = own.shape[2]
    half = columns // 2
    column_sums[...] = jnp.zeros_like(column_sums)

    def step(index, carry):
        for upper in range(2):
            first = pl.multiple_of(index * TILE + upper * half, TILE)
            rows_t = own[0, :, pl.ds(first, TILE)].T
            target = lax.rem(tile[0] + upper, 2) * half
            partial = strip_totals(rows_t, other.at[0], target, half, column_sums, False)
            row_out[0, :, pl.ds(first, TILE)] = row_vector(partial)
        return carry

    lax.fori_loop(0, half // TILE, step, 0)
    column_out[0] = jnp.sum(column_sums[...], axis=0, keepdims=True)


def diagonal_totals(own):
    count, depth, columns = own.shape
    pairs = columns * columns // 2
    extended = columns + columns // 2 + TILE
    total = pl.pallas_call(
        diagonal_kernel,
        grid=(count,),
        out_shape=jax.ShapeDtypeStruct((count, 1, columns), jnp.float32),
        in_specs=[pl.BlockSpec((1, depth, columns), lambda w: (w, 0, 0))],
        out_specs=pl.BlockSpec((1, 1, columns), lambda w: (w, 0, 0)),
        scratch_shapes=[
            pltpu.VMEM((depth, extended), own.dtype),
            pltpu.VMEM((SUBLANES, extended), jnp.float32),
        ],
        cost_estimate=pl.CostEstimate(
            flops=count * pairs * 512, bytes_accessed=own.size * 2, transcendentals=0
        ),
    )(own)
    return total.reshape(count, columns)


def cross_totals(tile, own, other):
    count, depth, columns = own.shape
    pairs = columns * columns // 2
    block = pl.BlockSpec((1, depth, columns), lambda w, *_: (w, 0, 0))
    line = pl.BlockSpec((1, 1, columns), lambda w, *_: (w, 0, 0))
    row_part, column_part = pl.pallas_call(
        cross_kernel,
        out_shape=[jax.ShapeDtypeStruct((count, 1, columns), jnp.float32)] * 2,
        grid_spec=pltpu.PrefetchScalarGridSpec(
            num_scalar_prefetch=1,
            grid=(count,),
            in_specs=[block, block],
            out_specs=[line, line],
            scratch_shapes=[pltpu.VMEM((SUBLANES, columns), jnp.float32)],
        ),
        cost_estimate=pl.CostEstimate(
            flops=count * pairs * 512, bytes_accessed=own.size * 4, transcendentals=0
        ),
    )(tile, own, other)
    return row_part.reshape(count, columns), column_part.reshape(count, columns)


def local_windows(tick_bars, prior_bars):
    groups = lax.axis_size("tm")
    group_cols = ASSETS // (2 * groups)
    series = jnp.concatenate(
        [prior_bars.reshape(-1, group_cols), tick_bars.reshape(-1, group_cols)], axis=0
    )
    return window_stack(series)


def shards(tick_bars, prior_bars):
    groups = lax.axis_size("tm")
    outgoing = local_windows(tick_bars, prior_bars)
    arrived = lax.all_to_all(outgoing, "tm", split_axis=0, concat_axis=0, tiled=True)
    arrived = arrived.reshape(groups, WIN_DEV, DEPTH, -1)
    scaled = jnp.transpose(arrived, (1, 2, 0, 3)).reshape(WIN_DEV, DEPTH, -1)
    partner = swapped(scaled, "asset", 0)
    tile = lax.axis_index("asset").astype(jnp.int32).reshape(1)
    diagonal_part = diagonal_totals(scaled)
    row_part, column_part = cross_totals(tile, scaled, partner)
    returned = swapped(column_part.astype(jnp.bfloat16), "asset", 0).astype(jnp.float32)
    totals = diagonal_part + row_part + returned
    return totals * (math.sqrt(SPAN) / ASSETS)


def solution(mesh):
    in_specs = (P("asset", "tm", None), P("asset", "tm", None))
    out_specs = P("tm", "asset")
    return jax.shard_map(shards, mesh=mesh, in_specs=in_specs, out_specs=out_specs, check_vma=False)
```

```python
import functools
import math

import jax
import jax.numpy as jnp
from jax import lax
from jax.experimental import pallas as pl
from jax.experimental.pallas import tpu as pltpu
from jax.sharding import PartitionSpec as P

ASSETS = 8192
SPAN = 30
STRIDE = 5
WIN_DEV = 3
LEAD = 25
DEPTH = 32
TILE = 256
LANES = 128
SUBLANES = 8


FLOOR_SQUARES = 1.0


def cycle_next(time, tile):
    core = time % 2
    along = (1 + core + tile) % 2
    return time + along * (1 - 2 * core), tile + (1 - along) * (1 - 2 * tile)


def around(block, forward):
    times, tiles = lax.axis_size("tm"), lax.axis_size("asset")
    route = []
    for time in range(times):
        for tile in range(tiles):
            next_time, next_tile = cycle_next(time, tile)
            hop = (time * tiles + tile, next_time * tiles + next_tile)
            route.append(hop if forward else hop[::-1])
    return lax.ppermute(block, ("tm", "asset"), route)


def window_stack(extended):
    columns = extended.shape[1]
    count = (extended.shape[0] - SPAN) // STRIDE + 1
    groups = extended.reshape(-1, STRIDE, columns)
    stacked = jnp.stack(
        [groups[offset : offset + count] for offset in range(SPAN // STRIDE)], axis=1
    )
    values = stacked.reshape(count, SPAN, columns)
    centred = values - jnp.mean(values, axis=1, keepdims=True)
    squares = jnp.sum(centred * centred, axis=1, keepdims=True)
    scaled = (centred * lax.rsqrt(jnp.maximum(squares, FLOOR_SQUARES))).astype(jnp.bfloat16)
    return jnp.pad(scaled, ((0, 0), (0, DEPTH - SPAN), (0, 0)))


def strip_totals(rows, source, first, count, column_sums, own_first):
    groups, _, width = source.shape
    rows_t = rows.T
    row_partial = jnp.zeros((width, LANES), jnp.float32)
    for offset in range(count):
        group = lax.rem(first + offset, groups)
        magnitude = jnp.abs(jnp.dot(rows_t, source[group], preferred_element_type=jnp.float32))
        for lane in range(0, width, LANES):
            row_partial = row_partial + magnitude[:, lane : lane + LANES]
        if offset or not own_first:
            folded = jnp.sum(magnitude.reshape(width // SUBLANES, SUBLANES, width), axis=0)
            column_sums[group] = column_sums[group] + folded
    return jnp.sum(row_partial.T, axis=0, keepdims=True)


def diagonal(source, out, column_sums):
    groups = source.shape[0]
    half = groups // 2
    column_sums[...] = jnp.zeros_like(column_sums)

    def step(index, carry):
        out[index, 0] = strip_totals(source[index], source, index, half + 1, column_sums, True)
        later = index + half
        out[later, 0] = strip_totals(source[later], source, later, half, column_sums, True)
        return carry

    lax.fori_loop(0, half, step, 0)
    out[:, 0] = out[:, 0] + jnp.sum(column_sums[...], axis=1, keepdims=True)


def totals_kernel(crosses, own, other, own_out, other_out, column_sums):
    groups = own.shape[0]

    @pl.when(crosses[0] == 1)
    def _():
        column_sums[...] = jnp.zeros_like(column_sums)

        def step(index, carry):
            own_out[index, 0] = strip_totals(own[index], other, 0, groups, column_sums, False)
            return carry

        lax.fori_loop(0, groups, step, 0)
        other_out[:, 0] = jnp.sum(column_sums[...], axis=1, keepdims=True)

    @pl.when(crosses[0] == 0)
    def _():
        diagonal(own, own_out, column_sums)
        diagonal(other, other_out, column_sums)


def pair_totals(crosses, own, other):
    groups, depth, width = own.shape
    block = pl.BlockSpec((groups, DEPTH, width), lambda w, *_: (0, w, 0))
    line = pl.BlockSpec((groups, 1, 1, width), lambda w, *_: (0, w, 0, 0))
    return pl.pallas_call(
        totals_kernel,
        out_shape=[jax.ShapeDtypeStruct((groups, depth // DEPTH, 1, width), jnp.float32)] * 2,
        grid_spec=pltpu.PrefetchScalarGridSpec(
            num_scalar_prefetch=1,
            grid=(depth // DEPTH,),
            in_specs=[block, block],
            out_specs=[line, line],
            scratch_shapes=[pltpu.VMEM((groups, SUBLANES, width), jnp.float32)],
        ),
    )(crosses, own, other)


def windows_kernel(tick, prior, out, series):
    width = series.shape[1]
    lead = prior.shape[1] // width
    for row in range(lead):
        series[row : row + 1] = prior[:, row * width : (row + 1) * width]
    for row in range(tick.shape[1] // width):
        series[lead + row : lead + row + 1] = tick[:, row * width : (row + 1) * width]
    for window in range(out.shape[0] * WIN_DEV):
        values = series[window * STRIDE : window * STRIDE + SPAN]
        centred = values - jnp.sum(values, axis=0, keepdims=True) * (1.0 / SPAN)
        squares = jnp.sum(centred * centred, axis=0, keepdims=True)
        scaled = centred * lax.rsqrt(jnp.maximum(squares, FLOOR_SQUARES))
        scaled = jnp.concatenate([scaled, jnp.zeros((DEPTH - SPAN, width), jnp.float32)], axis=0)
        first = window % WIN_DEV * DEPTH
        out[window // WIN_DEV, first : first + DEPTH] = scaled.astype(jnp.bfloat16)


def deliver_kernel(groups, outgoing, own, other, own_send, own_recv, next_send, next_recv, local_sem):
    time = lax.axis_index("tm")
    tile = lax.axis_index("asset")
    next_time, next_tile = cycle_next(time, tile)
    barrier = pltpu.get_barrier_semaphore()
    for step in range(1, groups):
        peer = lax.rem(time + step, groups)
        pl.semaphore_signal(
            barrier, inc=1, device_id=(peer, tile), device_id_type=pl.DeviceIdType.MESH
        )
    pl.semaphore_signal(
        barrier, inc=1, device_id=(time, 1 - tile), device_id_type=pl.DeviceIdType.MESH
    )
    pl.semaphore_wait(barrier, groups)

    def send(step):
        peer = lax.rem(time + step, groups)
        return pltpu.make_async_remote_copy(
            src_ref=outgoing.at[peer],
            dst_ref=own.at[time],
            send_sem=own_send.at[step],
            recv_sem=own_recv.at[step],
            device_id=(peer, tile),
            device_id_type=pl.DeviceIdType.MESH,
        )

    def forward(step):
        source = lax.rem(time - step + groups, groups)
        return pltpu.make_async_remote_copy(
            src_ref=own.at[source],
            dst_ref=other.at[source],
            send_sem=next_send.at[source],
            recv_sem=next_recv.at[source],
            device_id=(next_time, next_tile),
            device_id_type=pl.DeviceIdType.MESH,
        )

    sends = [send(step) for step in range(1, groups)]
    for copy in sends:
        copy.start()
    local = pltpu.make_async_copy(outgoing.at[time], own.at[time], local_sem)
    local.start()
    local.wait()
    forwards = [forward(step) for step in range(groups)]
    forwards[0].start()
    for step in range(1, groups):
        sends[step - 1].wait_recv()
        forwards[step].start()
    for copy in sends:
        copy.wait_send()
    for group in range(groups):
        arrival = pltpu.make_async_remote_copy(
            src_ref=own.at[group],
            dst_ref=other.at[group],
            send_sem=next_send.at[group],
            recv_sem=next_recv.at[group],
            device_id=(next_time, next_tile),
            device_id_type=pl.DeviceIdType.MESH,
        )
        arrival.wait()


def delivered(outgoing):
    groups = outgoing.shape[0]
    vmem = pl.BlockSpec(memory_space=pltpu.VMEM)
    return pl.pallas_call(
        functools.partial(deliver_kernel, groups),
        out_shape=[jax.ShapeDtypeStruct(outgoing.shape, outgoing.dtype)] * 2,
        in_specs=[vmem],
        out_specs=[vmem, vmem],
        scratch_shapes=[pltpu.SemaphoreType.DMA((groups,))] * 4 + [pltpu.SemaphoreType.DMA],
        compiler_params=pltpu.CompilerParams(collective_id=0, has_side_effects=True),
    )(outgoing)


def local_windows(tick_bars, prior_bars):
    groups = lax.axis_size("tm")
    width = ASSETS // (2 * groups)
    ticks, prior = tick_bars.reshape(1, -1), prior_bars.reshape(1, -1)
    if width % LANES:
        series = jnp.concatenate([prior.reshape(-1, width), ticks.reshape(-1, width)], axis=0)
        return window_stack(series).reshape(groups, WIN_DEV * DEPTH, width)
    rows = (ticks.size + prior.size) // width
    return pl.pallas_call(
        windows_kernel,
        out_shape=jax.ShapeDtypeStruct((groups, WIN_DEV * DEPTH, width), jnp.bfloat16),
        scratch_shapes=[pltpu.VMEM((-(-rows // SUBLANES) * SUBLANES, width), jnp.float32)],
    )(ticks, prior)


def retiled(blocks):
    groups, depth, width = blocks.shape
    if width % LANES == 0:
        return blocks
    join = TILE // width
    grouped = blocks.reshape(groups // join, join, depth, width)
    return jnp.transpose(grouped, (0, 2, 1, 3)).reshape(groups // join, depth, TILE)


def shards(tick_bars, prior_bars):
    own, other = delivered(local_windows(tick_bars, prior_bars))
    own, other = retiled(own), retiled(other)
    core = lax.axis_index("tm") % 2
    crosses = (core == lax.axis_index("asset")).astype(jnp.int32).reshape(1)
    own_part, other_part = pair_totals(crosses, own, other)
    own_part = jnp.transpose(own_part[:, :, 0], (1, 0, 2)).reshape(WIN_DEV, -1)
    other_part = jnp.transpose(other_part[:, :, 0], (1, 0, 2)).reshape(WIN_DEV, -1)
    returned = around(other_part.astype(jnp.bfloat16), False).astype(jnp.float32)
    return (own_part + returned) * (math.sqrt(SPAN) / ASSETS)


def solution(mesh):
    in_specs = (P("asset", "tm", None), P("asset", "tm", None))
    out_specs = P("tm", "asset")
    return jax.shard_map(shards, mesh=mesh, in_specs=in_specs, out_specs=out_specs, check_vma=False)
```

```python
import functools
import math

import jax
import jax.numpy as jnp
from jax import lax
from jax.experimental import pallas as pl
from jax.experimental.pallas import tpu as pltpu
from jax.sharding import PartitionSpec as P

ASSETS = 8192
SPAN = 30
STRIDE = 5
WIN_DEV = 3
LEAD = 25
DEPTH = 32
TILE = 256
LANES = 128
SUBLANES = 8
PART_SCALE = 256.0


FLOOR_SQUARES = 1.0


def cycle_next(time, tile):
    core = time % 2
    along = (1 + core + tile) % 2
    return time + along * (1 - 2 * core), tile + (1 - along) * (1 - 2 * tile)


def around(block, forward):
    times, tiles = lax.axis_size("tm"), lax.axis_size("asset")
    route = []
    for time in range(times):
        for tile in range(tiles):
            next_time, next_tile = cycle_next(time, tile)
            hop = (time * tiles + tile, next_time * tiles + next_tile)
            route.append(hop if forward else hop[::-1])
    return lax.ppermute(block, ("tm", "asset"), route)


def window_stack(extended):
    columns = extended.shape[1]
    count = (extended.shape[0] - SPAN) // STRIDE + 1
    groups = extended.reshape(-1, STRIDE, columns)
    stacked = jnp.stack(
        [groups[offset : offset + count] for offset in range(SPAN // STRIDE)], axis=1
    )
    values = stacked.reshape(count, SPAN, columns)
    centred = values - jnp.mean(values, axis=1, keepdims=True)
    squares = jnp.sum(centred * centred, axis=1, keepdims=True)
    scaled = (centred * lax.rsqrt(jnp.maximum(squares, FLOOR_SQUARES))).astype(jnp.bfloat16)
    return jnp.pad(scaled, ((0, 0), (0, DEPTH - SPAN), (0, 0)))


def split_parts(block):
    scaled = block.astype(jnp.float32) * PART_SCALE
    high = scaled.astype(jnp.float8_e4m3fn).astype(jnp.float32)
    return high, scaled - high


def right_parts(block):
    high, low = split_parts(block)
    return jnp.concatenate([high, high, low, low], axis=0).astype(jnp.float8_e4m3fn)


def strip_totals(rows, source, first, count, column_sums, own_first):
    groups, _, width = source.shape
    high, low = split_parts(rows)
    rows_t = jnp.concatenate([high, low, high, low], axis=0).T.astype(jnp.float8_e4m3fn)
    row_partial = jnp.zeros((width, LANES), jnp.float32)
    for offset in range(count):
        group = lax.rem(first + offset, groups)
        magnitude = jnp.abs(jnp.dot(rows_t, source[group], preferred_element_type=jnp.float32))
        for lane in range(0, width, LANES):
            row_partial = row_partial + magnitude[:, lane : lane + LANES]
        if offset or not own_first:
            folded = jnp.sum(magnitude.reshape(width // SUBLANES, SUBLANES, width), axis=0)
            column_sums[group] = column_sums[group] + folded
    return jnp.sum(row_partial.T, axis=0, keepdims=True)


def fill_parts(source, parts):
    def fill(group, carry):
        parts[group] = right_parts(source[group])
        return carry

    lax.fori_loop(0, source.shape[0], fill, 0)


def diagonal(source, out, column_sums, parts):
    groups = source.shape[0]
    half = groups // 2
    fill_parts(source, parts)
    column_sums[...] = jnp.zeros_like(column_sums)

    def step(index, carry):
        out[index, 0] = strip_totals(source[index], parts, index, half + 1, column_sums, True)
        later = index + half
        out[later, 0] = strip_totals(source[later], parts, later, half, column_sums, True)
        return carry

    lax.fori_loop(0, half, step, 0)
    out[:, 0] = out[:, 0] + jnp.sum(column_sums[...], axis=1, keepdims=True)


def totals_kernel(crosses, own, other, own_out, other_out, column_sums, parts):
    groups = own.shape[0]

    @pl.when(crosses[0] == 1)
    def _():
        fill_parts(other, parts)
        column_sums[...] = jnp.zeros_like(column_sums)

        def step(index, carry):
            own_out[index, 0] = strip_totals(own[index], parts, 0, groups, column_sums, False)
            return carry

        lax.fori_loop(0, groups, step, 0)
        other_out[:, 0] = jnp.sum(column_sums[...], axis=1, keepdims=True)

    @pl.when(crosses[0] == 0)
    def _():
        diagonal(own, own_out, column_sums, parts)
        diagonal(other, other_out, column_sums, parts)


def pair_totals(crosses, own, other):
    groups, depth, width = own.shape
    block = pl.BlockSpec((groups, DEPTH, width), lambda w, *_: (0, w, 0))
    line = pl.BlockSpec((groups, 1, 1, width), lambda w, *_: (0, w, 0, 0))
    return pl.pallas_call(
        totals_kernel,
        out_shape=[jax.ShapeDtypeStruct((groups, depth // DEPTH, 1, width), jnp.float32)] * 2,
        grid_spec=pltpu.PrefetchScalarGridSpec(
            num_scalar_prefetch=1,
            grid=(depth // DEPTH,),
            in_specs=[block, block],
            out_specs=[line, line],
            scratch_shapes=[
                pltpu.VMEM((groups, SUBLANES, width), jnp.float32),
                pltpu.VMEM((groups, 4 * DEPTH, width), jnp.float8_e4m3fn),
            ],
        ),
    )(crosses, own, other)


def windows_kernel(tick, prior, out, series):
    width = series.shape[1]
    lead = prior.shape[1] // width
    for row in range(lead):
        series[row : row + 1] = prior[:, row * width : (row + 1) * width]
    for row in range(tick.shape[1] // width):
        series[lead + row : lead + row + 1] = tick[:, row * width : (row + 1) * width]
    for window in range(out.shape[0] * WIN_DEV):
        values = series[window * STRIDE : window * STRIDE + SPAN]
        centred = values - jnp.sum(values, axis=0, keepdims=True) * (1.0 / SPAN)
        squares = jnp.sum(centred * centred, axis=0, keepdims=True)
        scaled = centred * lax.rsqrt(jnp.maximum(squares, FLOOR_SQUARES))
        scaled = jnp.concatenate([scaled, jnp.zeros((DEPTH - SPAN, width), jnp.float32)], axis=0)
        first = window % WIN_DEV * DEPTH
        out[window // WIN_DEV, first : first + DEPTH] = scaled.astype(jnp.bfloat16)


def deliver_kernel(groups, outgoing, own, other, own_send, own_recv, next_send, next_recv, local_sem):
    time = lax.axis_index("tm")
    tile = lax.axis_index("asset")
    next_time, next_tile = cycle_next(time, tile)
    barrier = pltpu.get_barrier_semaphore()
    for step in range(1, groups):
        peer = lax.rem(time + step, groups)
        pl.semaphore_signal(
            barrier, inc=1, device_id=(peer, tile), device_id_type=pl.DeviceIdType.MESH
        )
    pl.semaphore_signal(
        barrier, inc=1, device_id=(time, 1 - tile), device_id_type=pl.DeviceIdType.MESH
    )
    pl.semaphore_wait(barrier, groups)

    def send(step):
        peer = lax.rem(time + step, groups)
        return pltpu.make_async_remote_copy(
            src_ref=outgoing.at[peer],
            dst_ref=own.at[time],
            send_sem=own_send.at[step],
            recv_sem=own_recv.at[step],
            device_id=(peer, tile),
            device_id_type=pl.DeviceIdType.MESH,
        )

    def forward(step):
        source = lax.rem(time - step + groups, groups)
        return pltpu.make_async_remote_copy(
            src_ref=own.at[source],
            dst_ref=other.at[source],
            send_sem=next_send.at[source],
            recv_sem=next_recv.at[source],
            device_id=(next_time, next_tile),
            device_id_type=pl.DeviceIdType.MESH,
        )

    sends = [send(step) for step in range(1, groups)]
    for copy in sends:
        copy.start()
    local = pltpu.make_async_copy(outgoing.at[time], own.at[time], local_sem)
    local.start()
    local.wait()
    forwards = [forward(step) for step in range(groups)]
    forwards[0].start()
    for step in range(1, groups):
        sends[step - 1].wait_recv()
        forwards[step].start()
    for copy in sends:
        copy.wait_send()
    for group in range(groups):
        arrival = pltpu.make_async_remote_copy(
            src_ref=own.at[group],
            dst_ref=other.at[group],
            send_sem=next_send.at[group],
            recv_sem=next_recv.at[group],
            device_id=(next_time, next_tile),
            device_id_type=pl.DeviceIdType.MESH,
        )
        arrival.wait()


def delivered(outgoing):
    groups = outgoing.shape[0]
    vmem = pl.BlockSpec(memory_space=pltpu.VMEM)
    return pl.pallas_call(
        functools.partial(deliver_kernel, groups),
        out_shape=[jax.ShapeDtypeStruct(outgoing.shape, outgoing.dtype)] * 2,
        in_specs=[vmem],
        out_specs=[vmem, vmem],
        scratch_shapes=[pltpu.SemaphoreType.DMA((groups,))] * 4 + [pltpu.SemaphoreType.DMA],
        compiler_params=pltpu.CompilerParams(collective_id=0, has_side_effects=True),
    )(outgoing)


def local_windows(tick_bars, prior_bars):
    groups = lax.axis_size("tm")
    width = ASSETS // (2 * groups)
    ticks, prior = tick_bars.reshape(1, -1), prior_bars.reshape(1, -1)
    if width % LANES:
        series = jnp.concatenate([prior.reshape(-1, width), ticks.reshape(-1, width)], axis=0)
        return window_stack(series).reshape(groups, WIN_DEV * DEPTH, width)
    rows = (ticks.size + prior.size) // width
    return pl.pallas_call(
        windows_kernel,
        out_shape=jax.ShapeDtypeStruct((groups, WIN_DEV * DEPTH, width), jnp.bfloat16),
        scratch_shapes=[pltpu.VMEM((-(-rows // SUBLANES) * SUBLANES, width), jnp.float32)],
    )(ticks, prior)


def retiled(blocks):
    groups, depth, width = blocks.shape
    if width % LANES == 0:
        return blocks
    join = TILE // width
    grouped = blocks.reshape(groups // join, join, depth, width)
    return jnp.transpose(grouped, (0, 2, 1, 3)).reshape(groups // join, depth, TILE)


def shards(tick_bars, prior_bars):
    own, other = delivered(local_windows(tick_bars, prior_bars))
    own, other = retiled(own), retiled(other)
    core = lax.axis_index("tm") % 2
    crosses = (core == lax.axis_index("asset")).astype(jnp.int32).reshape(1)
    own_part, other_part = pair_totals(crosses, own, other)
    own_part = jnp.transpose(own_part[:, :, 0], (1, 0, 2)).reshape(WIN_DEV, -1)
    other_part = jnp.transpose(other_part[:, :, 0], (1, 0, 2)).reshape(WIN_DEV, -1)
    returned = around(other_part, False)
    return (own_part + returned) * (math.sqrt(SPAN) / (ASSETS * PART_SCALE * PART_SCALE))


def solution(mesh):
    in_specs = (P("asset", "tm", None), P("asset", "tm", None))
    out_specs = P("tm", "asset")
    return jax.shard_map(shards, mesh=mesh, in_specs=in_specs, out_specs=out_specs, check_vma=False)
```
